256 devices in a mesh: row: 16 (over y, x), col: 16 (over z, core).
Axes of the slice: x: 4, y: 4, z: 8, core: 2. Of those that a mesh axis runs over, the one named last changes fastest.
Arguments:
- eigenbasis: bfloat16 [16384, 16384], P('row', 'col'), may hold values from -0.046875 to 0.046875
- gradient: float32 [16384, 2048], P('row', 'col'), may hold values from -6 to 6
- moment_one: float32 [16384, 2048], P('col', 'row'), may hold values from -0.6 to 0.6
- moment_two: float32 [16384, 2048], P('col', 'row'), may hold values from 0.0001 to 0.01
Outputs:
- update: float32 [16384, 2048], P('row', 'col')
- new_one: float32 [16384, 2048], P('col', 'row')
- new_two: float32 [16384, 2048], P('col', 'row')
The draws below stay inside these ranges and needn't reach their ends.
All inputs are finite; a program needn't handle non-finite values.
Results may differ from the reference program's by a relative error of at most 0.004.
Values may be sent and summed in bfloat16 or wider, within the bound.
No kernel may reach another device: no remote copies, remote signals or barrier semaphores. Data moves between devices by JAX's collectives and lax.ppermute only.
A program may use at most 64 MiB of HBM per device.

```python
import math
import jax
import jax.numpy as jnp

D = 16384
COLS = 2048


def spiked(entries, own_key, source, target, parts, factor):
    owner, partner = [(jnp.arange(entries.shape[position]) // (entries.shape[position] // parts)).reshape([-1 if axis == position else 1 for axis in range(entries.ndim)]) for position in (source, target)]
    chosen = jax.random.permutation(own_key, parts)[partner]
    strong = (owner == chosen) | (owner == (partner + parts // 2) % parts)
    return jnp.where(strong, factor * entries, entries)


def block_scale(own_key, extent, split, low, high):
    def one(position, blocks):
        heights = jax.random.uniform(jax.random.fold_in(jax.random.fold_in(own_key, 6), position), (blocks,), jnp.float32, low / len(split), high / len(split))
        return jnp.repeat(jnp.exp(heights), extent[position] // blocks).reshape((-1,) + (1,) * (len(extent) - position - 1))

    level = one(*split[0])
    for cut in split[1:]:
        level = level * one(*cut)
    return level


def scatter_about(own_key, dims, scale, reach, split=(), dtype=jnp.bfloat16):
    loudness = block_scale(own_key, dims, split, -0.22, 0.18) if split else 1.0
    array = jax.random.normal(own_key, dims, jnp.float32) * scale * loudness
    return jnp.minimum(jnp.maximum(array, -reach), reach).astype(dtype)


def heavy_noise(key, extent, width, limit, split, heavy, held_as=jnp.bfloat16):
    result = width * jax.random.normal(key, extent, jnp.float32)
    if split:
        result = result * block_scale(key, extent, split, -0.22, 0.18)
    return jnp.clip(spiked(result, jax.random.fold_in(key, 3), *heavy), -limit, limit).astype(held_as)


def setup_inputs(seed: int = 0) -> dict:
    key_of = jax.random.split(jax.random.key(seed), 5)
    return {
        "eigenbasis": scatter_about(key_of[0], (D, D), D ** -0.5, 0.046875, ((0, 16), (1, 16))),
        "gradient": heavy_noise(key_of[1], (D, COLS), 1.0, 6.0, ((0, 16), (1, 16)), (0, 1, 16, 2.0), jnp.float32),
        "moment_one": scatter_about(key_of[2], (D, COLS), 0.1, 0.6, ((0, 16), (1, 16)), jnp.float32),
        "moment_two": jnp.clip(jnp.exp(math.log(0.01) - 4.6051702 * jax.random.uniform(key_of[3], (D, COLS), jnp.float32) ** block_scale(key_of[3], (D, COLS), ((0, 16), (1, 16)), -0.2, 0.2)), 0.0001, 0.01),
    }


beta_one = 0.9
beta_two = 0.999
step_count = 10
epsilon = 1e-08

def reference(eigenbasis, gradient, moment_one, moment_two):
    grad_half = gradient.astype(jnp.bfloat16)
    rotated = jnp.dot(eigenbasis.T, grad_half, preferred_element_type=jnp.float32)
    new_one = beta_one * moment_one + (1.0 - beta_one) * rotated
    new_two = beta_two * moment_two + (1.0 - beta_two) * rotated * rotated
    corr_one = 1.0 - beta_one ** step_count
    corr_two = 1.0 - beta_two ** step_count
    direction = (new_one / corr_one / (jnp.sqrt(new_two / corr_two) + epsilon)).astype(jnp.bfloat16)
    update = jnp.dot(eigenbasis, direction, preferred_element_type=jnp.float32)
    return (update, new_one, new_two)
```

```python
import jax
import jax.numpy as jnp
from jax import lax
from jax.sharding import Mesh, PartitionSpec as P

beta_one = 0.9
beta_two = 0.999
step_count = 10
epsilon = 1e-08

CHUNKS = 2
f32 = jnp.float32
bf16 = jnp.bfloat16


def shift(value, axis, by):
    n = lax.axis_size(axis)
    return lax.ppermute(value, axis, [(i, (i + by) % n) for i in range(n)])


def put(buf, piece, *index):
    start = [0 if i is None else i for i in index] + [0] * (buf.ndim - len(index))
    shape = [buf.shape[d] if i is None else 1 for d, i in enumerate(index)]
    shape += list(piece.shape[len(piece.shape) - (buf.ndim - len(index)):])
    return lax.dynamic_update_slice(buf, piece.reshape(shape), start)


def gather_z(own):
    h = own.shape[0]
    z = lax.axis_index("z")
    buf = put(jnp.zeros((8, *own.shape), own.dtype), own, z)
    right = left = own
    for s in range(1, 4):
        right, left = shift(right, "z", 1), shift(left, "z", -1)
        buf = put(put(buf, right, (z - s) % 8), left, (z + s) % 8)
    far = jnp.concatenate(
        [shift(right[: h // 2], "z", 1), shift(left[h // 2 :], "z", -1)]
    )
    buf = put(buf, far, (z + 4) % 8)
    return jnp.stack([buf, shift(buf, "core", 1)])


def sum_at(pick, axis):
    i = lax.axis_index(axis)
    total = pick(i).astype(f32)
    for d in (2, 1, 3):
        total = total + shift(pick((i + d) % 4).astype(bf16), axis, d).astype(f32)
    return total


def scatter_xy(part):
    core, x, y = (lax.axis_index(a) for a in ("core", "x", "y"))
    h = part.shape[3]
    first, second = part[:, :, :, : h // 2], part[:, :, :, h // 2 :]

    def at_x(value, ix):
        v = lax.dynamic_index_in_dim(value, (ix % 2) ^ core, 0, False)
        return lax.dynamic_index_in_dim(v, ix // 2, v.ndim - 3, False)

    one = sum_at(lambda i: at_x(first, i), "x")
    two = sum_at(lambda i: lax.dynamic_index_in_dim(second, i, 1, False), "y")
    one = sum_at(lambda i: lax.dynamic_index_in_dim(one, i, 0, False), "y")
    two = sum_at(lambda i: at_x(two, i), "x")
    return jnp.concatenate([one, two])


def gather_xy(own):
    h = own.shape[0]
    x, y = lax.axis_index("x"), lax.axis_index("y")

    def along(piece, axis):
        i = lax.axis_index(axis)
        buf = put(jnp.zeros((4, *piece.shape), piece.dtype), piece, i)
        for d in (1, 3, 2):
            buf = put(buf, shift(piece, axis, d), (i - d) % 4)
        return buf

    one, two = along(own[: h // 2], "x"), along(own[h // 2 :], "y")
    one, two = along(one, "y"), along(two, "x")
    return one, two


def scatter_z(one, two):
    core, z = lax.axis_index("core"), lax.axis_index("z")
    hh, k = one.shape[2], one.shape[3]
    one = one.reshape(8, 2, hh, k)
    two = two.reshape(2, 2, 4, hh, k).transpose(2, 0, 1, 3, 4).reshape(8, 2, hh, k)
    both = jnp.concatenate([one, two], axis=2)
    mine = lax.dynamic_index_in_dim(both, core, 1, False)
    other = lax.dynamic_index_in_dim(both, 1 - core, 1, False)
    v = mine.astype(f32) + shift(other, "core", 1).astype(f32)

    def at(o):
        return lax.dynamic_index_in_dim(v, (z + o) % 8, 0, False)

    right = shift(at(4)[:hh].astype(bf16), "z", 1)
    left = shift(at(4)[hh:].astype(bf16), "z", -1)
    zero = jnp.zeros((hh, k), f32)
    right = at(3) + jnp.concatenate([right.astype(f32), zero])
    left = at(-3) + jnp.concatenate([zero, left.astype(f32)])
    for s in (2, 1, 0):
        right = shift(right.astype(bf16), "z", 1).astype(f32)
        left = shift(left.astype(bf16), "z", -1).astype(f32)
        if s:
            right, left = at(s) + right, at(-s) + left
    return at(0) + right + left


def local(eigenbasis, gradient, moment_one, moment_two):
    rows = 128 // CHUNKS
    grad = gradient.T.astype(bf16)
    one_t, two_t = moment_one.T, moment_two.T
    corr_one = 1.0 - beta_one**step_count
    corr_two = 1.0 - beta_two**step_count
    ones, twos, updates = [], [], []
    for j in range(CHUNKS):
        cut = slice(j * rows, (j + 1) * rows)
        with jax.named_scope(f"a{j}"):
            whole = gather_z(grad[cut])
        with jax.named_scope(f"b{j}"):
            part = lax.dot_general(
                whole.reshape(16 * rows, -1), eigenbasis, (((1,), (0,)), ((), ())), preferred_element_type=f32
            ).astype(bf16)
            rotated = scatter_xy(part.reshape(2, 4, 2, rows, -1))
        with jax.named_scope(f"m{j}"):
            new_one = beta_one * one_t[cut] + (1.0 - beta_one) * rotated
            new_two = beta_two * two_t[cut] + (1.0 - beta_two) * rotated * rotated
            direction = (new_one / corr_one / (jnp.sqrt(new_two / corr_two) + epsilon)).astype(bf16)
        with jax.named_scope(f"c{j}"):
            halves = gather_xy(direction)
        with jax.named_scope(f"d{j}"):
            back = [
                lax.dot_general(
                    half.reshape(16 * rows // 2, -1), eigenbasis, (((1,), (1,)), ((), ())), preferred_element_type=f32
                ).astype(bf16).reshape(4, 4, rows // 2, -1)
                for half in halves
            ]
            updates.append(scatter_z(*back))
        ones.append(new_one)
        twos.append(new_two)
    return tuple(jnp.concatenate(parts).T for parts in (updates, ones, twos))


def solution(mesh):
    fine = Mesh(mesh.devices.reshape(4, 4, 8, 2), ("y", "x", "z", "core"))
    row, col = ("y", "x"), ("z", "core")
    return jax.shard_map(
        local,
        mesh=fine,
        in_specs=(P(row, col), P(row, col), P(col, row), P(col, row)),
        out_specs=(P(row, col), P(col, row), P(col, row)),
        check_vma=False,
    )
```

```python
import functools

import jax
import jax.numpy as jnp
from jax import lax
from jax.experimental import pallas as pl
from jax.experimental.pallas import tpu as pltpu
from jax.sharding import Mesh, PartitionSpec as P

beta_one = 0.9
beta_two = 0.999
step_count = 10
epsilon = 1e-08

CHUNKS = 2
AXES = ("y", "x", "z", "core")
f32 = jnp.float32
bf16 = jnp.bfloat16


def permute(value, to):
    pairs = []
    for i in range(256):
        y, x, z, c = i // 64, i // 16 % 4, i // 2 % 8, i % 2
        y, x, z, c = to(y, x, z, c)
        pairs.append((i, ((y % 4 * 4 + x % 4) * 8 + z % 8) * 2 + c))
    return lax.ppermute(value, AXES, pairs)


def swap(value):
    return permute(value, lambda y, x, z, c: (y, x, z, 1 - c))


def ring(value):
    return permute(value, lambda y, x, z, c: (y, x, z + 1 - 2 * c, c))


def across(value, stage, d):
    return permute(value, lambda y, x, z, c: (y, x + d, z, c) if c == stage else (y + d, x, z, c))


def where_am_i():
    return tuple(lax.axis_index(a) for a in AXES)


def table_one():
    y, x, z, core = where_am_i()
    offset = jnp.array([0, 1, 2, 3, -1, -2, -3, 4], jnp.int32) * jnp.where(core == 0, -1, 1)
    b = 2 * ((z + offset[:, None] + 16) % 8) + jnp.arange(2, dtype=jnp.int32)[None]
    by, bx = b // 4, b % 4
    place = jnp.where(core == 0, 4 * ((bx - x + 4) % 4) + by, 4 * ((by - y + 4) % 4) + bx)
    return jnp.concatenate([place.reshape(16), jnp.full((1,), core, jnp.int32)]).astype(jnp.int32)


def table_two():
    y, x, z, core = where_am_i()
    u = jnp.arange(32, dtype=jnp.int32)
    d2, d1, half = u // 8, u // 2 % 4, u % 2
    dx, dy = jnp.where(core == 0, d1, d2), jnp.where(core == 0, d2, d1)
    b = 4 * ((y - dy + 4) % 4) + (x - dx + 4) % 4
    o, c = (b // 2 - z + 8) % 8, b % 2
    a = jnp.minimum(o, 8 - o)
    keep = jnp.where(a == 0, c == core, jnp.where(a == 4, half == core, (o > 4) == (core == 1)))
    unit = jnp.where(a == 0, 14 + half, jnp.where(a == 4, c, 14 - 4 * a + 2 * c + half))
    return (unit + 16 * keep.astype(jnp.int32)).astype(jnp.int32)


def call(kernel, name, table, operands, outs, scratch, flops):
    size = sum(a.size * a.dtype.itemsize for a in (*operands, *outs))
    return pl.pallas_call(
        kernel,
        name=name,
        out_shape=outs,
        in_specs=[pl.BlockSpec(memory_space=pltpu.SMEM)]
        + [pl.BlockSpec(memory_space=pltpu.VMEM)] * len(operands),
        out_specs=[pl.BlockSpec(memory_space=pltpu.VMEM)] * len(outs),
        scratch_shapes=scratch,
        cost_estimate=pl.CostEstimate(flops=flops, bytes_accessed=size, transcendentals=0),
        compiler_params=pltpu.CompilerParams(vmem_limit_bytes=32 * 2**20),
    )(table, *operands)


def forward_kernel(table, own, r1, r2, r3, s1, s2, s3, r4, s4, basis, o2, o1, o3, o0, lhs):
    half, k = lhs.shape[1:]
    for c in range(2):
        for piece, ref in enumerate((own, r1, r2, r3, s1, s2, s3)):
            lhs[pl.ds(2 * table[2 * piece + c], 2)] = ref[c].reshape(2, half, k)
        place = 2 * table[14 + c]
        lhs[place + table[16]] = r4[c]
        lhs[place + 1 - table[16]] = s4[c]
    for d, out in ((2, o2), (1, o1), (3, o3), (0, o0)):
        rows = lhs[8 * d : 8 * d + 8].reshape(8 * half, k)
        out[...] = jnp.dot(rows, basis[...], preferred_element_type=f32).astype(out.dtype).reshape(out.shape)


def back_kernel(table, f0, f1, f2, f3, basis, send, keep, lhs):
    half, m = lhs.shape[1:]
    for d2, ref in enumerate((f0, f1, f2, f3)):
        for d1 in range(4):
            for h in range(2):
                lhs[table[8 * d2 + 2 * d1 + h]] = ref[d1, h * half : (h + 1) * half]
    for out, first in ((send, 0), (keep, 16)):
        for t in range(2):
            rows = lhs[first + 8 * t : first + 8 * t + 8].reshape(8 * half, m)
            part = lax.dot_general(rows, basis[...], (((1,), (1,)), ((), ())), preferred_element_type=f32)
            out[8 * t : 8 * t + 8] = part.astype(out.dtype).reshape(8, half, -1)


def sum_kernel(mine, p0, p1, p2, p3, o2, o1, o3, o0):
    for d, out in ((2, o2), (1, o1), (3, o3), (0, o0)):
        i = lax.rem(mine[0] + d, 4)
        total = p0[i] + p1[i].astype(f32) + p2[i].astype(f32) + p3[i].astype(f32)
        out[...] = total.astype(out.dtype)


def gather_z(own):
    core = lax.axis_index("core")
    h = own.shape[0] // 2
    other = swap(own)
    piece = jnp.where(core == 0, jnp.stack([own, other]), jnp.stack([other, own]))
    rings, swaps = [piece], []
    for s in range(3):
        rings.append(ring(rings[-1]))
        swaps.append(swap(rings[-1]))
    last = ring(lax.dynamic_slice_in_dim(rings[-1], core * h, h, 1))
    return (*rings, *swaps, last, swap(last))


def scatter_z(send, keep):
    core = lax.axis_index("core")
    h, k = send.shape[1:]
    v = keep + swap(send).astype(f32)
    first = ring(v[0:2].astype(bf16)).astype(f32)
    zero = jnp.zeros_like(first)
    total = jnp.where(core == 0, jnp.concatenate([first, zero], 1), jnp.concatenate([zero, first], 1))
    for at in (2, 6, 10):
        total = v[at : at + 4].reshape(2, 2 * h, k) + total
        total = ring(total.astype(bf16)).astype(f32)
    mine = lax.dynamic_index_in_dim(total, core, 0, False)
    given = lax.dynamic_index_in_dim(total, 1 - core, 0, False).astype(bf16)
    return v[14:].reshape(2 * h, k) + mine + swap(given).astype(f32)


def local(eigenbasis, gradient, moment_one, moment_two):
    rows = 128 // CHUNKS
    half = rows // 2
    grad = gradient.T.astype(bf16)
    one_t, two_t = moment_one.T, moment_two.T
    corr_one = 1.0 - beta_one**step_count
    corr_two = 1.0 - beta_two**step_count
    y, x, z, core = where_am_i()
    place_one, place_two = table_one(), table_two()
    mine = jnp.where(core == 0, y, x).astype(jnp.int32).reshape(1)
    S = jax.ShapeDtypeStruct
    flops = 2 * 16 * rows * 1024 * 1024
    ones, twos, updates = [], [], []
    for j in range(CHUNKS):
        cut = slice(j * rows, (j + 1) * rows)
        with jax.named_scope(f"a{j}"):
            pieces = gather_z(grad[cut])
        with jax.named_scope(f"b{j}"):
            big, small = S((4, rows, 1024), bf16), S((rows, 1024), bf16)
            p2, p1, p3, p0 = call(
                forward_kernel, f"forward{j}", place_one, (*pieces, eigenbasis),
                (big, big, big, S((4, rows, 1024), f32)), [pltpu.VMEM((32, half, 1024), bf16)], flops,
            )
            p2, p1, p3 = across(p2, 0, 2), across(p1, 0, 1), across(p3, 0, 3)
            q2, q1, q3, q0 = call(
                sum_kernel, f"sum{j}", mine, (p0, p1, p2, p3), (small, small, small, S((rows, 1024), f32)), [],
                16 * rows * 1024,
            )
            q2, q1, q3 = across(q2, 1, 2), across(q1, 1, 1), across(q3, 1, 3)
            rotated = q0 + q1.astype(f32) + q2.astype(f32) + q3.astype(f32)
        with jax.named_scope(f"m{j}"):
            new_one = beta_one * one_t[cut] + (1.0 - beta_one) * rotated
            new_two = beta_two * two_t[cut] + (1.0 - beta_two) * rotated * rotated
            direction = (new_one / corr_one / (jnp.sqrt(new_two / corr_two) + epsilon)).astype(bf16)
        with jax.named_scope(f"c{j}"):
            line = jnp.stack([direction, *(across(direction, 0, d) for d in (1, 2, 3))])
            lines = (line, *(across(line, 1, d) for d in (1, 2, 3)))
        with jax.named_scope(f"d{j}"):
            send, keep = call(
                back_kernel, f"back{j}", place_two, (*lines, eigenbasis),
                (S((16, half, 1024), bf16), S((16, half, 1024), f32)), [pltpu.VMEM((32, half, 1024), bf16)], flops,
            )
            updates.append(scatter_z(send, keep))
        ones.append(new_one)
        twos.append(new_two)
    return tuple(jnp.concatenate(parts).T for parts in (updates, ones, twos))


def solution(mesh):
    fine = Mesh(mesh.devices.reshape(4, 4, 8, 2), AXES)
    row, col = ("y", "x"), ("z", "core")
    return jax.shard_map(
        local,
        mesh=fine,
        in_specs=(P(row, col), P(row, col), P(col, row), P(col, row)),
        out_specs=(P(row, col), P(col, row), P(col, row)),
        check_vma=False,
    )
```

```python
import jax
import jax.numpy as jnp
from jax import lax
from jax.experimental import pallas as pl
from jax.experimental.pallas import tpu as pltpu
from jax.sharding import Mesh, PartitionSpec as P


beta_one = 0.9
beta_two = 0.999
step_count = 10
epsilon = 1e-08

CHUNKS = 2
ROWS = 32
HALF = 64
TILE = 256
AXES = ("y", "x", "z", "core")
f32 = jnp.float32
bf16 = jnp.bfloat16


def permute(value, to):
    pairs = []
    for i in range(256):
        y, x, z, c = i // 64, i // 16 % 4, i // 2 % 8, i % 2
        y, x, z, c = to(y, x, z, c)
        pairs.append((i, ((y % 4 * 4 + x % 4) * 8 + z % 8) * 2 + c))
    return lax.ppermute(value, AXES, pairs)


def swap(value):
    return permute(value, lambda y, x, z, c: (y, x, z, 1 - c))


def up(value):
    return permute(value, lambda y, x, z, c: (y, x, z + 1, c))


def down(value):
    return permute(value, lambda y, x, z, c: (y, x, z - 1, c))


def across(value, stage, d, flip):
    return permute(value, lambda y, x, z, c: (y, x + d, z, c) if c ^ flip == stage else (y + d, x, z, c))


def where_am_i():
    return tuple(lax.axis_index(a) for a in AXES)


def table_one(flip):
    y, x, z, core = where_am_i()
    offset = jnp.array([0, -1, -2, -3, 1, 2, 3, 4], jnp.int32)
    b = 2 * ((z + offset[:, None] + 16) % 8) + jnp.arange(2, dtype=jnp.int32)[None]
    by, bx = b // 4, b % 4
    place = jnp.where(core == flip, 4 * ((bx - x + 4) % 4) + by, 4 * ((by - y + 4) % 4) + bx)
    return place.reshape(16).astype(jnp.int32)


def table_two(flip):
    y, x, z, core = where_am_i()
    u = jnp.arange(16, dtype=jnp.int32)
    d2, d1 = u // 4, u % 4
    dx, dy = jnp.where(core == flip, d1, d2), jnp.where(core == flip, d2, d1)
    b = 4 * ((y - dy + 4) % 4) + (x - dx + 4) % 4
    return (2 * ((b // 2 - z + 8) % 8) + b % 2).astype(jnp.int32)


def call(kernel, table, operands, outs, scratch, flops):
    size = sum(a.size * a.dtype.itemsize for a in (*operands, *outs))
    return pl.pallas_call(
        kernel,
        out_shape=outs,
        in_specs=[pl.BlockSpec(memory_space=pltpu.SMEM)]
        + [pl.BlockSpec(memory_space=pltpu.VMEM)] * len(operands),
        out_specs=[pl.BlockSpec(memory_space=pltpu.VMEM)] * len(outs),
        scratch_shapes=scratch,
        cost_estimate=pl.CostEstimate(flops=flops, bytes_accessed=size, transcendentals=0),
        compiler_params=pltpu.CompilerParams(vmem_limit_bytes=24 * 2**20),
    )(table, *operands)


def forward_kernel(chunk):
    def kernel(table, *refs):
        pieces, (near, far, o2, o1, o3, o0, lhs) = refs[:8], refs[8:]
        for c in range(2):
            for piece, ref in enumerate(pieces):
                first = ROWS * chunk if piece < 7 else 0
                lhs[table[2 * piece + c]] = ref[c, first : first + ROWS]
        k = lhs.shape[2]
        for side, basis in enumerate((near, far)):

            @pl.loop(0, k // TILE)
            def _(t):
                at = pl.ds(pl.multiple_of(t * TILE, TILE), TILE)
                to = pl.ds(pl.multiple_of(side * k + t * TILE, TILE), TILE)
                part = jnp.dot(lhs[...].reshape(16 * ROWS, k), basis[:, at], preferred_element_type=f32)
                part = part.reshape(4, 4, ROWS, TILE)
                for d, out in ((2, o2), (1, o1), (3, o3), (0, o0)):
                    out[:, :, to] = part[d].astype(out.dtype)

    return kernel


def back_kernel(table, *refs):
    lines, (near, far, ends, ahead, behind, lhs) = refs[:8], refs[8:]
    for j in range(2):
        for d2, ref in enumerate(lines[4 * j : 4 * j + 4]):
            for d1 in range(4):
                lhs[table[16 * j + 4 * d2 + d1], j] = ref[d1]
    m = lhs.shape[3] // 2

    @pl.loop(0, m // TILE)
    def _(t):
        at = pl.ds(pl.multiple_of(t * TILE, TILE), TILE)
        dims = (((1,), (1,)), ((), ()))
        part = lax.dot_general(lhs[..., :m].reshape(32 * ROWS, m), near[at, :], dims, preferred_element_type=f32)
        part += lax.dot_general(lhs[..., m:].reshape(32 * ROWS, m), far[at, :], dims, preferred_element_type=f32)
        part = part.reshape(16, 2, ROWS, TILE)
        ends[0:2, :, :, at], ends[2:4, :, :, at] = part[0:2], part[8:10]
        ahead[:, :, :, at], behind[:, :, :, at] = part[2:8], part[10:16]


def sum_kernel(mine, p0, p1, p2, p3, o2, o1, o3, o0):
    @pl.loop(0, o0.shape[1] // TILE)
    def _(t):
        at = pl.ds(pl.multiple_of(t * TILE, TILE), TILE)
        for d, out in ((2, o2), (1, o1), (3, o3), (0, o0)):
            i = lax.rem(mine[0] + d, 4)
            total = p0[i, :, at].astype(f32) + p1[i, :, at].astype(f32)
            total += p2[i, :, at].astype(f32) + p3[i, :, at].astype(f32)
            out[:, at] = total.astype(out.dtype)


def adam_kernel(chunk):
    rows = slice(ROWS * chunk, ROWS * chunk + ROWS)
    corr_one = 1.0 - beta_one**step_count
    corr_two = 1.0 - beta_two**step_count

    def kernel(unused, q0, q1, q2, q3, near, other, new_near, new_other, direction):
        m = near.shape[2]
        for side, (old, new) in enumerate(((near, new_near), (other, new_other))):

            @pl.loop(0, m // TILE)
            def _(t):
                at = pl.ds(pl.multiple_of(t * TILE, TILE), TILE)
                to = pl.ds(pl.multiple_of(side * m + t * TILE, TILE), TILE)
                rotated = q0[:, to] + q1[:, to].astype(f32) + q2[:, to].astype(f32) + q3[:, to].astype(f32)
                first = beta_one * old[0, rows, at] + (1.0 - beta_one) * rotated
                second = beta_two * old[1, rows, at] + (1.0 - beta_two) * rotated * rotated
                new[0, :, at] = first
                new[1, :, at] = second
                direction[:, to] = (first / corr_one / (jnp.sqrt(second / corr_two) + epsilon)).astype(bf16)

    return kernel


def turn_in_kernel(core, one, two, mine, theirs):
    for i, ref in enumerate((one, two)):
        turned = ref[...].T
        low, high = turned[:HALF], turned[HALF:]
        mine[i] = jnp.where(core[0] == 0, low, high)
        theirs[i] = jnp.where(core[0] == 0, high, low)


def turn_kernel(core, near0, near1, given, new_one, new_two):
    for i, out in enumerate((new_one, new_two)):
        mine = jnp.concatenate([near0[i], near1[i]])
        theirs = jnp.concatenate([given[0, i], given[1, i]])
        low = core[0] == 0
        out[...] = jnp.concatenate([jnp.where(low, mine, theirs), jnp.where(low, theirs, mine)]).T


def halves(value, core, axis=0):
    cut = [lax.dynamic_slice_in_dim(value, HALF * c, HALF, axis) for c in (core, 1 - core)]
    return cut[0], cut[1]


def ordered(mine, theirs, core, axis=0):
    return jnp.where(core == 0, jnp.concatenate([mine, theirs], axis), jnp.concatenate([theirs, mine], axis))


def step(eigenbasis, gradient, moment_one, moment_two):
    y, x, _, core = where_am_i()
    S = jax.ShapeDtypeStruct
    nothing = jnp.zeros((1,), jnp.int32)
    flops = 2 * 16 * ROWS * 1024 * 2048

    mine, theirs = halves(gradient.T.astype(bf16), core)
    own = ordered(mine[None], swap(theirs)[None], core)
    ups, downs = [own], [own]
    for _ in range(3):
        ups.append(up(ups[-1]))
        downs.append(down(downs[-1]))
    far = (up(ups[3][:, :ROWS]), down(downs[3][:, ROWS:]))
    basis = (eigenbasis, swap(eigenbasis))
    which = core.astype(jnp.int32).reshape(1)
    near_m, theirs = call(
        turn_in_kernel, which, (moment_one, moment_two), (S((2, HALF, 1024), f32),) * 2, [],
        2000 * 128 * 1024,
    )
    far_m = swap(theirs)
    big, small = S((4, ROWS, 2048), bf16), S((ROWS, 2048), bf16)
    new = S((2, ROWS, 1024), f32)
    news, lines = [], []
    for j in range(CHUNKS):
        flip = j % 2
        p = dict(zip((2, 1, 3, 0), call(
            forward_kernel(j), table_one(flip), (*ups, *downs[1:], far[j], *basis),
            (big, big, big, S((4, ROWS, 2048), f32)), [pltpu.VMEM((16, ROWS, 1024), bf16)], flops,
        )))
        for d in (2, 1, 3):
            p[d] = across(p[d], 0, d, flip)
        index = jnp.where(core == flip, y, x).astype(jnp.int32).reshape(1)
        q = dict(zip((2, 1, 3, 0), call(
            sum_kernel, index, [p[d] for d in range(4)], (small, small, small, S((ROWS, 2048), f32)), [], 2000 * ROWS * 2048,
        )))
        for d in (2, 1, 3):
            q[d] = across(q[d], 1, d, flip)
        near, far_new, direction = call(
            adam_kernel(j), nothing, [*(q[d] for d in range(4)), near_m, far_m],
            (new, new, small), [], 2000 * ROWS * 2048,
        )
        news.append((near, far_new))
        line = jnp.stack([direction, *(across(direction, 0, d, flip) for d in (1, 2, 3))])
        lines += [line, *(across(line, 1, d, flip) for d in (1, 2, 3))]
    ends, ahead, behind = call(
        back_kernel, jnp.concatenate([table_two(0), table_two(1)]), (*lines, *basis),
        [S((n, 2, ROWS, 1024), f32) for n in (4, 6, 6)], [pltpu.VMEM((16, 2, ROWS, 2048), bf16)], 2 * flops,
    )

    at_up, at_down = ends[2:, 0], ends[2:, 1]
    for s in (1, 2, 3, 4):
        to_up = at_up.astype(bf16)
        to_down = at_down.astype(bf16)
        to_up, to_down = up(to_up), down(to_down)
        at_up = to_up.astype(f32)
        if s < 4:
            mine = ahead[6 - 2 * s : 8 - 2 * s]
            at_up = mine + at_up if s > 1 else mine.at[:, 0].add(at_up)
        at_down = to_down.astype(f32)
        if s < 4:
            mine = behind[2 * s - 2 : 2 * s]
            at_down = mine + at_down if s > 1 else mine.at[:, 1].add(at_down)
    total = ends[:2] + at_up + at_down
    mine = lax.dynamic_index_in_dim(total, core, 0, False).reshape(HALF, 1024)
    theirs = lax.dynamic_index_in_dim(total, 1 - core, 0, False).reshape(HALF, 1024)
    update = ordered(mine, swap(theirs), core).T

    given = swap(jnp.stack([news[0][1], news[1][1]]))
    turned = S((1024, 128), f32)
    new_one, new_two = call(
        turn_kernel, which, [news[0][0], news[1][0], given],
        (turned, turned), [], 2000 * 128 * 1024,
    )
    return update, new_one, new_two


def solution(mesh):
    fine = Mesh(mesh.devices.reshape(4, 4, 8, 2), AXES)
    row, col = ("y", "x"), ("z", "core")
    return jax.shard_map(
        step,
        mesh=fine,
        in_specs=(P(row, col), P(row, col), P(col, row), P(col, row)),
        out_specs=(P(row, col), P(col, row), P(col, row)),
        check_vma=False,
    )
```
